256 devices in a mesh: grp: 2 (over core), dp: 128 (over z, y, x).
Axes of the slice: x: 4, y: 4, z: 8, core: 2. Of those that a mesh axis runs over, the one named last changes fastest.
Arguments:
- version_tags: int32 [262144], P(('grp', 'dp')), may hold values from 0 to 3
- packed_pos: int32 [262144], P(('grp', 'dp')), may hold values from 0 to 262143, as said below
- valid_mask: int32 [262144, 128], P(('grp', 'dp')), may hold values from 0 to 1, as said below
- returns: float32 [262144, 128], P(('grp', 'dp')), may hold values from -16 to 16
- values: float32 [262144, 128], P(('grp', 'dp')), may hold values from -6 to 6
- log_ratio_new: float32 [262144, 128], P(('grp', 'dp')), may hold values from -4 to 4
- log_ratio_prox: float32 [262144, 128], P(('grp', 'dp')), may hold values from -4 to 4
Outputs:
- token_loss: float32 [262144, 128], P(('grp', 'dp'))
- block_loss: float32 [262144], P(('grp', 'dp'))
The draws below stay inside these ranges and needn't reach their ends.
Inputs may be any that keep to these rules, and one draw needn't show every extreme that they name: `packed_pos`: A permutation of the blocks. Blocks stay within their group of 128 devices along dp; each device's 1024 packed positions take 1024 // 128 blocks from every device of its group, those of the s-th device of the group at local packed positions s * (8) onward; which of a device's blocks go where is otherwise arbitrary. `valid_mask`: some blocks have no valid token.
All inputs are finite; a program needn't handle non-finite values.
Results may differ from the reference program's by a relative error of at most 0.00002.
Values sent between devices are 32-bit elements; how exact they have to be, the bound alone decides.
A program may use at most 64 MiB of HBM per device.

```python
import math
import jax
import jax.numpy as jnp
from jax import lax

BLOCK = 128
VERSIONS = 4
BLK_DEV = 1024
BLOCKS = 262144
N_GRP = 2
N_DP = 128


def common_tags(key):
    integer_draws = jax.random.randint(jax.random.fold_in(key, 101), (BLOCKS,), 0, 10)
    return (integer_draws >= 1).astype(jnp.int32) + (integer_draws >= 3).astype(jnp.int32) + (integer_draws >= 6).astype(jnp.int32)


def draw_version_tags(key, part):
    return common_tags(key)


def draw_valid_mask(key, part):
    token_draws = jax.random.randint(jax.random.fold_in(key, 404), (BLOCKS, BLOCK), 0, 4)
    block_draws = jax.random.randint(jax.random.fold_in(key, 405), (BLOCKS,), 0, 32)
    block_index = jnp.arange(BLOCKS, dtype=jnp.int32)
    emptied = jnp.logical_or(block_draws == 0, block_index % 997 == 0)
    keep_block = 1 - emptied.astype(jnp.int32)
    return ((token_draws >= 1).astype(jnp.int32) * keep_block[:, None]).astype(jnp.int32)


def draw_returns(key, part):
    labels = common_tags(key)
    subkeys = jax.random.split(jax.random.fold_in(key, 202), 4)
    onehot = (labels[:, None] == jnp.arange(VERSIONS, dtype=jnp.int32)[None, :]).astype(jnp.float32)
    position = jnp.arange(BLOCKS).astype(jnp.float32) / BLOCKS
    phase_shift = jax.random.uniform(subkeys[3], (), jnp.float32, 0.0, 2.0 * math.pi)
    offsets = jax.random.uniform(subkeys[0], (VERSIONS,), jnp.float32, -2.0, 2.0)
    scales = jnp.exp(jax.random.uniform(subkeys[1], (VERSIONS,), jnp.float32, math.log(0.5), math.log(2.0)))
    jitter = jax.random.truncated_normal(subkeys[2], -6.0, 6.0, (BLOCKS, BLOCK), jnp.float32)
    trend = jnp.sin(6.0 * math.pi * position + phase_shift)
    level = jnp.sum(onehot * offsets[None, :], axis=1) + trend
    spread = jnp.sum(onehot * scales[None, :], axis=1)
    return level[:, None] + spread[:, None] * jitter


def draw_packed_pos(key, part):
    per_peer = BLK_DEV // N_DP
    subkeys = jax.random.split(jax.random.fold_in(key, 303), N_GRP * N_DP)
    orders = jax.vmap(lambda subkey: jax.random.permutation(subkey, BLK_DEV))(subkeys).astype(jnp.int32)
    device = jnp.arange(N_GRP * N_DP, dtype=jnp.int32)[:, None]
    group_index = device // N_DP
    source = device % N_DP
    target = orders // per_peer
    slot_index = orders % per_peer
    packed = group_index * (BLK_DEV * N_DP) + target * BLK_DEV + source * per_peer + slot_index
    return packed.reshape(-1).astype(jnp.int32)


def level_of(own_key, extent, shards, low, high):
    def one(dim, shards_of):
        draws = jax.random.uniform(jax.random.fold_in(jax.random.fold_in(own_key, 6), dim), (shards_of,), jnp.float32, low / len(shards), high / len(shards))
        return jnp.repeat(jnp.exp(draws), extent[dim] // shards_of).reshape((-1,) + (1,) * (len(extent) - dim - 1))

    level = one(*shards[0])
    for cut in shards[1:]:
        level = level * one(*cut)
    return level


def bell_draw(own_key, extent, scale, reach, shards=(), held_as=jnp.bfloat16):
    array = jax.random.normal(own_key, extent, jnp.float32) * scale
    if len(shards) > 0:
        array = level_of(own_key, extent, shards, -0.22, 0.18) * array
    return jnp.clip(array, min=-reach, max=reach).astype(held_as)


def setup_inputs(seed: int = 0) -> dict:
    arg_keys = jax.random.split(jax.random.key(seed), 8)
    version_tags = draw_version_tags(jax.random.fold_in(arg_keys[7], 71), 0)
    packed_pos = draw_packed_pos(jax.random.fold_in(arg_keys[7], 71), 0)
    valid_mask = draw_valid_mask(jax.random.fold_in(arg_keys[7], 71), 0)
    returns = draw_returns(jax.random.fold_in(arg_keys[7], 71), 0)
    values = bell_draw(arg_keys[4], (BLOCKS, BLOCK), 1.0, 6.0, ((0, 256),), jnp.float32)
    log_ratio_new = bell_draw(arg_keys[5], (BLOCKS, BLOCK), 0.25, 4.0, ((0, 256),), jnp.float32)
    log_ratio_prox = bell_draw(arg_keys[6], (BLOCKS, BLOCK), 0.25, 4.0, ((0, 256),), jnp.float32)
    return dict(version_tags=version_tags, packed_pos=packed_pos, valid_mask=valid_mask, returns=returns, values=values, log_ratio_new=log_ratio_new, log_ratio_prox=log_ratio_prox)


def reference(version_tags, packed_pos, valid_mask, returns, values, log_ratio_new, log_ratio_prox):
    advantage = returns - values
    maskf = valid_mask.astype(jnp.float32)
    onehot = (version_tags[:, None] == jnp.arange(VERSIONS, dtype=jnp.int32)[None, :]).astype(jnp.float32)
    block_count = lax.optimization_barrier(jnp.sum(maskf, axis=1))
    counts = lax.optimization_barrier(jnp.sum(onehot * block_count[:, None], axis=0))
    adv_sums = lax.optimization_barrier(jnp.sum(onehot * lax.optimization_barrier(jnp.sum(maskf * advantage, axis=1))[:, None], axis=0))
    version_mean = adv_sums / jnp.maximum(counts, 1.0)
    block_mean = lax.optimization_barrier(jnp.sum(onehot * version_mean[None, :], axis=1))
    centered = advantage - block_mean[:, None]
    squares = lax.optimization_barrier(jnp.sum(onehot * lax.optimization_barrier(jnp.sum(maskf * centered * centered, axis=1))[:, None], axis=0))
    version_scale = 1.0 / jnp.sqrt(squares / jnp.maximum(counts, 1.0) + 0.05)
    white = centered * lax.optimization_barrier(jnp.sum(onehot * version_scale[None, :], axis=1))[:, None]
    prob_ratio = jnp.exp(log_ratio_new)
    weight = maskf * jnp.exp(log_ratio_prox)
    clipped = jnp.clip(prob_ratio, 0.8, 1.2)
    loss = -weight * jnp.minimum(prob_ratio * white, clipped * white)
    per_block = lax.optimization_barrier(jnp.sum(loss, axis=1)) / jnp.maximum(block_count, 1.0)
    token_loss = jnp.zeros_like(loss).at[packed_pos].set(loss)
    block_loss = jnp.zeros_like(per_block).at[packed_pos].set(per_block)
    return (token_loss, block_loss)
```

```python
import functools

import jax
import jax.numpy as jnp
from jax import lax
from jax.experimental import pallas as pl
from jax.experimental.pallas import tpu as pltpu
from jax.sharding import Mesh
from jax.sharding import PartitionSpec as P

MESH = pl.DeviceIdType.MESH
VERSIONS = 4
LANES = 128
AXES = ("grp", "z", "y", "x")
FAR4 = (2, 1, 3, 0)
FAR8 = (4, 3, 5, 2, 6, 1, 7, 0)


def split3(value):
    high = value.astype(jnp.bfloat16)
    rest = value - high.astype(jnp.float32)
    middle = rest.astype(jnp.bfloat16)
    low = (rest - middle.astype(jnp.float32)).astype(jnp.bfloat16)
    return high, middle, low


def combine(moments):
    count = sum(m[0] for m in moments)
    total = sum(m[0] * m[1] for m in moments)
    mean = total / jnp.maximum(count, 1.0)
    square = sum(m[2] + m[0] * (m[1] - mean) * (m[1] - mean) for m in moments)
    return count, mean, square


def total_of(array):
    return jnp.sum(jnp.sum(array, axis=0, keepdims=True), axis=1, keepdims=True)


def kernel(
    tags_h, packed_h, mask_h, returns_h, values_h, new_h, prox_h,
    token_o, block_o,
    tags, packed, mask, returns, values, new, prox,
    per_block, onehot, side, pieces, placed, loss,
    msg_a, msg_b, got_a, got_b,
    packed_count, got_count, count_rows, got_rows,
    load_sem, stat_send, stat_recv, count_send, count_recv, token_send, token_recv,
):
    g, z, y, x = (lax.axis_index(name) for name in AXES)
    n_z, n_y, n_x = (lax.axis_size(name) for name in AXES[1:])
    plane = n_y * n_x
    blocks = mask.shape[0]
    chunk = blocks // n_z
    per_peer = blocks // (n_z * plane)
    here = y * n_x + x
    me = z * plane + here

    loads = [
        pltpu.make_async_copy(src, dst, load_sem.at[i])
        for i, (src, dst) in enumerate(
            [(returns_h, returns), (values_h, values), (mask_h, mask), (tags_h, tags), (packed_h, packed), (new_h, new), (prox_h, prox)]
        )
    ]
    for load in loads:
        load.start()

    def at(dg, dz, dy, dx):
        return (g ^ dg, lax.rem(z + dz, n_z), lax.rem(y + dy, n_y), lax.rem(x + dx, n_x))

    near = [(dg, 0, dy, dx) for dg in (0, 1) for dy in FAR4 for dx in FAR4][:]
    near = [o for o in near if o != (0, 0, 0, 0)]
    line = [(0, dz, 0, 0) for dz in FAR8 if dz]

    barrier = pltpu.get_barrier_semaphore()
    for o in near + line:
        pl.semaphore_signal(barrier, inc=1, device_id=at(*o), device_id_type=MESH)

    for load in loads[:4]:
        load.wait()
    for s in range(n_z):
        rows = pl.ds(s * chunk, chunk)
        valid = mask[rows, :].astype(jnp.float32).T
        advantage = (returns[rows, :] - values[rows, :]).T
        count = jnp.sum(valid, axis=0, keepdims=True)
        mean = jnp.sum(valid * advantage, axis=0, keepdims=True) / jnp.maximum(count, 1.0)
        centred = advantage - mean
        per_block[0, s : s + 1, :] = count
        per_block[1, s : s + 1, :] = mean
        per_block[2, s : s + 1, :] = jnp.sum(valid * centred * centred, axis=0, keepdims=True)

    lane = lax.broadcasted_iota(jnp.int32, (1, LANES), 1)
    tag = tags[...]
    count, mean, square = per_block[0], per_block[1], per_block[2]
    local = [jnp.zeros((1, LANES), jnp.float32)] * 3
    for v in range(VERSIONS):
        mine = tag == v
        count_v = total_of(jnp.where(mine, count, 0.0))
        mean_v = total_of(jnp.where(mine, count * mean, 0.0)) / jnp.maximum(count_v, 1.0)
        square_v = total_of(jnp.where(mine, square + count * (mean - mean_v) * (mean - mean_v), 0.0))
        local = [jnp.where(lane == v, new_value, old) for new_value, old in zip((count_v, mean_v, square_v), local)]
    own_a = g * plane + here
    for k in range(3):
        msg_a[k] = local[k]
        got_a[own_a, k] = local[k]

    pl.semaphore_wait(barrier, len(near) + len(line))
    for o in near:
        pltpu.make_async_remote_copy(
            src_ref=msg_a, dst_ref=got_a.at[own_a], send_sem=stat_send.at[0], recv_sem=stat_recv.at[0],
            device_id=at(*o), device_id_type=MESH,
        ).start()

    def bytes_of(ref, send, recv):
        return pltpu.make_async_remote_copy(src_ref=ref, dst_ref=ref, send_sem=send, recv_sem=recv, device_id=(g, z, y, x), device_id_type=MESH)

    all_a = bytes_of(got_a.at[pl.ds(0, len(near))], stat_send.at[0], stat_recv.at[0])
    all_a.wait_recv()
    merged = combine([[got_a[i, k] for k in range(3)] for i in range(2 * plane)])
    for k in range(3):
        msg_b[k] = merged[k]
        got_b[z, k] = merged[k]
    for o in line:
        pltpu.make_async_remote_copy(
            src_ref=msg_b, dst_ref=got_b.at[z], send_sem=stat_send.at[1], recv_sem=stat_recv.at[1],
            device_id=at(*o), device_id_type=MESH,
        ).start()

    loads[4].wait()
    where = packed[...]
    target = lax.rem(where // blocks, n_z * plane)
    order = target * per_peer + lax.rem(where, blocks) - me * per_peer
    for s in range(n_z):
        rows = pl.ds(s * chunk, chunk)
        tag_rows = jnp.broadcast_to(tag[s : s + 1, :].astype(jnp.float32), (chunk, LANES)).T
        count_cols = jnp.broadcast_to(count[s : s + 1, :], (chunk, LANES)).T
        side[rows, 0:LANES] = tag_rows.astype(jnp.bfloat16)
        side[rows, LANES : 2 * LANES] = count_cols.astype(jnp.bfloat16)

    tag_at, min_at, max_at, adv_at = 0, 1, 2, 3

    @pl.loop(0, n_z)
    def _(c):
        rows = pl.ds(pl.multiple_of(c * chunk, chunk), chunk)
        slot = lax.broadcasted_iota(jnp.int32, (chunk, LANES), 0) + c * chunk
        for s in range(n_z):
            hit = jnp.broadcast_to(order[s : s + 1, :], (chunk, LANES)) == slot
            onehot[rows, s * LANES : (s + 1) * LANES] = jnp.where(hit, 1.0, 0.0).astype(jnp.bfloat16)
        moved = jnp.dot(onehot[rows, :], side[...], preferred_element_type=jnp.float32)
        placed[tag_at, rows, :] = moved[:, 0:LANES]
        packed_count[pl.ds(c, 1), :] = moved[:, LANES : 2 * LANES].T[0:1, :]

    for o in near:
        if o[0] == 0:
            pltpu.make_async_remote_copy(
                src_ref=packed_count, dst_ref=got_count.at[here], send_sem=count_send.at[0], recv_sem=count_recv.at[0],
                device_id=at(*o), device_id_type=MESH,
            ).start()
    got_count[here] = packed_count[...]

    for load in loads[5:]:
        load.wait()

    @pl.loop(0, n_z)
    def _(s):
        rows = pl.ds(pl.multiple_of(s * chunk, chunk), chunk)
        ratio = jnp.exp(new[rows, :])
        weight = mask[rows, :].astype(jnp.float32) * jnp.exp(prox[rows, :])
        parts = split3(weight * jnp.minimum(ratio, 1.2))
        parts += split3(weight * jnp.maximum(ratio, 0.8))
        parts += split3(returns[rows, :] - values[rows, :])
        for k, part in enumerate(parts):
            pieces[rows, k * LANES : (k + 1) * LANES] = part

    @pl.loop(0, n_z)
    def _(c):
        rows = pl.ds(pl.multiple_of(c * chunk, chunk), chunk)
        moved = jnp.dot(onehot[rows, :], pieces[...], preferred_element_type=jnp.float32)
        for k in range(3):
            high, middle, low = (moved[:, (3 * k + i) * LANES : (3 * k + i + 1) * LANES] for i in range(3))
            placed[min_at + k, rows, :] = high + middle + low

    bytes_of(got_count.at[pl.ds(0, plane - 1)], count_send.at[0], count_recv.at[0]).wait_recv()
    lanes8 = lax.broadcasted_iota(jnp.int32, (n_z, LANES), 1) // per_peer
    gathered = jnp.zeros((n_z, LANES), jnp.float32)
    for p in range(plane):
        turn = lax.rem((p - here + plane) * per_peer, LANES)
        gathered = jnp.where(lanes8 == p, pltpu.roll(got_count[p], turn, 1), gathered)
    for r in range(n_z):
        count_rows[r] = gathered[r : r + 1, :]
    got_rows[z] = count_rows[z]
    for o in line:
        device = at(*o)
        pltpu.make_async_remote_copy(
            src_ref=count_rows.at[device[1]], dst_ref=got_rows.at[z], send_sem=count_send.at[1], recv_sem=count_recv.at[1],
            device_id=device, device_id_type=MESH,
        ).start()

    all_b = bytes_of(got_b.at[pl.ds(0, len(line))], stat_send.at[1], stat_recv.at[1])
    all_b.wait_recv()
    count, mean, square = combine([[got_b[i, k] for k in range(3)] for i in range(n_z)])
    scale = 1.0 / jnp.sqrt(square / jnp.maximum(count, 1.0) + 0.05)

    def spread(row, v):
        return jnp.broadcast_to(jnp.sum(jnp.where(lane == v, row, 0.0), axis=1, keepdims=True), (chunk, LANES))

    means = [spread(mean, v) for v in range(VERSIONS)]
    scales = [spread(scale, v) for v in range(VERSIONS)]

    @pl.loop(0, n_z)
    def _(c):
        rows = pl.ds(pl.multiple_of(c * chunk, chunk), chunk)
        tag_c = placed[tag_at, rows, :]
        mean_c, scale_c = means[0], scales[0]
        for v in range(1, VERSIONS):
            mean_c = jnp.where(tag_c == v, means[v], mean_c)
            scale_c = jnp.where(tag_c == v, scales[v], scale_c)
        white = (placed[adv_at, rows, :] - mean_c) * scale_c
        factor = jnp.where(white >= 0.0, placed[min_at, rows, :], placed[max_at, rows, :])
        loss[rows, :] = -(factor * white)

    own = pl.ds(pl.multiple_of(me * per_peer, per_peer), per_peer)
    for dy in FAR4:
        for dx in FAR4:
            for dz in FAR8:
                if (dz, dy, dx) != (0, 0, 0):
                    device = at(0, dz, dy, dx)
                    there = (device[1] * plane + device[2] * n_x + device[3]) * per_peer
                    pltpu.make_async_remote_copy(
                        src_ref=loss.at[pl.ds(pl.multiple_of(there, per_peer), per_peer)], dst_ref=token_o.at[own],
                        send_sem=token_send, recv_sem=token_recv.at[z], device_id=device, device_id_type=MESH,
                    ).start()
    token_o[own, :] = loss[own, :]

    bytes_of(got_rows.at[pl.ds(0, len(line))], count_send.at[1], count_recv.at[1]).wait_recv()
    for dz in (0, 1, 7, 2, 6, 3, 5, 4):
        src = lax.rem(z + dz, n_z)
        expect = blocks // n_z - (per_peer if dz == 0 else 0)
        bytes_of(token_o.at[pl.ds(0, expect)], token_send, token_recv.at[src]).wait_recv()
        rows = pl.ds(pl.multiple_of(src * chunk, chunk), chunk)
        sums = jnp.sum(token_o[rows, :].T, axis=0, keepdims=True)
        block_o[pl.ds(src, 1), :] = sums / jnp.maximum(got_rows[src], 1.0)

    bytes_of(got_a.at[pl.ds(0, len(near))], stat_send.at[0], stat_recv.at[0]).wait_send()
    bytes_of(got_b.at[pl.ds(0, len(line))], stat_send.at[1], stat_recv.at[1]).wait_send()
    bytes_of(got_count.at[pl.ds(0, plane - 1)], count_send.at[0], count_recv.at[0]).wait_send()
    bytes_of(got_rows.at[pl.ds(0, len(line))], count_send.at[1], count_recv.at[1]).wait_send()
    bytes_of(token_o.at[pl.ds(0, blocks - per_peer)], token_send, token_recv.at[0]).wait_send()


def on_device(version_tags, packed_pos, valid_mask, returns, values, log_ratio_new, log_ratio_prox):
    blocks, tokens = valid_mask.shape
    n_z, n_y, n_x = (lax.axis_size(name) for name in AXES[1:])
    plane = n_y * n_x
    f32, i32, bf16 = jnp.float32, jnp.int32, jnp.bfloat16
    vmem, dma = pltpu.VMEM, pltpu.SemaphoreType.DMA
    small = (blocks // LANES, LANES)
    token_loss, block_loss = pl.pallas_call(
        kernel,
        out_shape=(pltpu.VMEM((blocks, tokens), f32), pltpu.VMEM(small, f32)),
        in_specs=[pl.BlockSpec(memory_space=pltpu.HBM)] * 7,
        out_specs=[pl.BlockSpec(memory_space=pltpu.VMEM)] * 2,
        scratch_shapes=[
            vmem(small, i32), vmem(small, i32), vmem((blocks, tokens), i32),
            *[vmem((blocks, tokens), f32)] * 4,
            vmem((3, *small), f32), vmem((blocks, blocks), bf16), vmem((blocks, 2 * LANES), bf16), vmem((blocks, 9 * LANES), bf16),
            vmem((4, blocks, LANES), f32), vmem((blocks, LANES), f32),
            vmem((3, 1, LANES), f32), vmem((3, 1, LANES), f32), vmem((2 * plane, 3, 1, LANES), f32), vmem((n_z, 3, 1, LANES), f32),
            vmem(small, f32), vmem((plane, *small), f32), vmem((n_z, 1, LANES), f32), vmem((n_z, 1, LANES), f32),
            dma((7,)), dma((2,)), dma((2,)), dma((2,)), dma((2,)), dma, dma((n_z,)),
        ],
        compiler_params=pltpu.CompilerParams(collective_id=0, has_side_effects=True, vmem_limit_bytes=32 * 2**20),
    )(*[pltpu.with_memory_space_constraint(a, pltpu.HBM) for a in (version_tags.reshape(small), packed_pos.reshape(small), valid_mask, returns, values, log_ratio_new, log_ratio_prox)])
    return token_loss, block_loss.reshape(blocks)


def solution(mesh):
    split = Mesh(mesh.devices.reshape(mesh.shape["grp"], 8, 4, 4), AXES)
    row, flat = P(AXES, None), P(AXES)
    return jax.shard_map(
        on_device,
        mesh=split,
        in_specs=(flat, flat, row, row, row, row, row),
        out_specs=(row, flat),
        check_vma=False,
    )
```

```python
import functools

import jax
import jax.numpy as jnp
from jax import lax
from jax.experimental import pallas as pl
from jax.experimental.pallas import tpu as pltpu
from jax.sharding import Mesh
from jax.sharding import PartitionSpec as P

MESH = pl.DeviceIdType.MESH
VERSIONS = 4
LANES = 128
AXES = ("grp", "z", "y", "x")
FAR4 = (2, 1, 3, 0)
FAR8 = (4, 3, 5, 2, 6, 1, 7, 0)


def combine(moments):
    count = sum(m[0] for m in moments)
    total = sum(m[0] * m[1] for m in moments)
    mean = total / jnp.maximum(count, 1.0)
    square = sum(m[2] + m[0] * (m[1] - mean) * (m[1] - mean) for m in moments)
    return count, mean, square


def total_of(array):
    return jnp.sum(jnp.sum(array, axis=0, keepdims=True), axis=1, keepdims=True)


def kernel(
    tags_h, packed_h, mask_h, returns_h, values_h, new_h, prox_h,
    token_o, block_o,
    tags, packed, mask, returns, values, new, prox,
    per_block, per_count, keys, kinds, placed, loss, inverse_v, inverse,
    msg_a, msg_b, got_a, got_b,
    packed_count, got_count, count_rows, got_rows,
    here_sem, part_sem, load_sem, scalar_sem, stat_send, stat_recv, count_send, count_recv, token_send, token_recv,
):
    g, z, y, x = (lax.axis_index(name) for name in AXES)
    n_z, n_y, n_x = (lax.axis_size(name) for name in AXES[1:])
    plane = n_y * n_x
    blocks = mask.shape[0]
    chunk = blocks // n_z
    per_peer = blocks // (n_z * plane)
    here = y * n_x + x
    me = z * plane + here

    parts = 4
    part = blocks // parts
    stat_loads = [
        [
            pltpu.make_async_copy(src.at[pl.ds(i * part, part)], dst.at[pl.ds(i * part, part)], part_sem.at[3 * i + k])
            for k, (src, dst) in enumerate([(mask_h, mask), (returns_h, returns), (values_h, values)])
        ]
        for i in range(parts)
    ]
    loads = [
        pltpu.make_async_copy(src, dst, load_sem.at[i])
        for i, (src, dst) in enumerate([(tags_h, tags), (packed_h, packed), (new_h, new), (prox_h, prox)])
    ]
    for load in sum(stat_loads, []) + loads[:2]:
        load.start()

    def at(dg, dz, dy, dx):
        return (g ^ dg, lax.rem(z + dz, n_z), lax.rem(y + dy, n_y), lax.rem(x + dx, n_x))

    flat = [(dg, 0, dy, dx) for dy in FAR4 for dx in FAR4 for dg in (1, 0) if (dg, dy, dx) != (0, 0, 0)]
    half = n_z // 2
    low = z < half

    def along(bits):
        return (g, z ^ bits, y, x)

    barrier = pltpu.get_barrier_semaphore()
    for o in flat:
        pl.semaphore_signal(barrier, inc=1, device_id=at(*o), device_id_type=MESH)
    for bits in range(1, half):
        pl.semaphore_signal(barrier, inc=1, device_id=along(bits), device_id_type=MESH)

    @pl.when(low)
    def _():
        for bits in range(half, n_z):
            pl.semaphore_signal(barrier, inc=1, device_id=along(bits), device_id_type=MESH)

    for s in range(n_z):
        rows = pl.ds(s * chunk, chunk)
        if s * chunk % part == 0:
            for load in stat_loads[s * chunk // part]:
                load.wait()
        valid = mask[rows, :].T
        per_count[s : s + 1, :] = jnp.sum(valid, axis=0, keepdims=True)
        valid = valid.astype(jnp.float32)
        advantage = (returns[rows, :] - values[rows, :]).T
        count = per_count[s : s + 1, :].astype(jnp.float32)
        mean = jnp.sum(valid * advantage, axis=0, keepdims=True) / jnp.maximum(count, 1.0)
        centred = advantage - mean
        per_block[0, s : s + 1, :] = count
        per_block[1, s : s + 1, :] = mean
        per_block[2, s : s + 1, :] = jnp.sum(valid * centred * centred, axis=0, keepdims=True)

    for load in loads[2:]:
        load.start()
    loads[0].wait()
    lane = lax.broadcasted_iota(jnp.int32, (1, LANES), 1)
    tag = tags[...]
    count, mean, square = per_block[0], per_block[1], per_block[2]
    local = [jnp.zeros((1, LANES), jnp.float32)] * 3
    for v in range(VERSIONS):
        mine = tag == v
        count_v = total_of(jnp.where(mine, count, 0.0))
        mean_v = total_of(jnp.where(mine, count * mean, 0.0)) / jnp.maximum(count_v, 1.0)
        square_v = total_of(jnp.where(mine, square + count * (mean - mean_v) * (mean - mean_v), 0.0))
        local = [jnp.where(lane == v, new_value, old) for new_value, old in zip((count_v, mean_v, square_v), local)]
    own_a = g * plane + here
    for k in range(3):
        msg_a[k] = local[k]
        got_a[own_a, k] = local[k]

    pl.semaphore_wait(barrier, len(flat) + half - 1 + jnp.where(low, 0, half))
    for o in flat:
        pltpu.make_async_remote_copy(
            src_ref=msg_a, dst_ref=got_a.at[own_a], send_sem=stat_send.at[0], recv_sem=stat_recv.at[0],
            device_id=at(*o), device_id_type=MESH,
        ).start()

    def bytes_of(ref, send, recv):
        return pltpu.make_async_remote_copy(src_ref=ref, dst_ref=ref, send_sem=send, recv_sem=recv, device_id=(g, z, y, x), device_id_type=MESH)

    @pl.when(jnp.logical_not(low))
    def _():
        for bits in range(half, n_z):
            pl.semaphore_signal(here_sem, inc=1, device_id=along(bits), device_id_type=MESH)

    loads[1].wait()
    where = packed[...]
    order = ((where // blocks) & (n_z * plane - 1)) * per_peer + (where & (blocks - 1)) - me * per_peer
    block = lax.broadcasted_iota(jnp.int32, order.shape, 0) * LANES + lax.broadcasted_iota(jnp.int32, order.shape, 1)
    value = block + blocks * (per_count[...] + 2 * LANES * tag)

    def columns(row):
        return jnp.broadcast_to(row, (chunk, LANES)).T

    for s in range(n_z):
        rows = pl.ds(s * chunk, chunk)
        keys[0, rows, :] = columns(order[s : s + 1, :])
        keys[1, rows, :] = columns(value[s : s + 1, :])
    place = lax.broadcasted_iota(jnp.int32, (chunk, LANES), 1)
    for c in range(n_z):
        total = jnp.zeros((chunk, LANES), jnp.int32)
        for s in range(n_z):
            rows = pl.ds(s * chunk, chunk)
            total = total + jnp.where(keys[0, rows, :] == place + c * LANES, keys[1, rows, :], 0)
        total = jnp.sum(total, axis=0, keepdims=True)
        inverse_v[c : c + 1, :] = total & (blocks - 1)
        packed_count[c : c + 1, :] = ((total // blocks) & (2 * LANES - 1)).astype(jnp.float32)
        kinds[c * chunk : (c + 1) * chunk, :] = columns((total // (2 * LANES * blocks)).astype(jnp.float32))
    to_scalar = pltpu.make_async_copy(inverse_v, inverse, scalar_sem)
    to_scalar.start()

    for load in loads[2:]:
        load.wait()
    for s in range(n_z):
        rows = pl.ds(s * chunk, chunk)
        ratio = jnp.exp(new[rows, :])
        weight = mask[rows, :].astype(jnp.float32) * jnp.exp(prox[rows, :])
        new[rows, :] = weight * jnp.minimum(ratio, 1.2)
        prox[rows, :] = weight * jnp.maximum(ratio, 0.8)
        returns[rows, :] = returns[rows, :] - values[rows, :]

    to_scalar.wait()
    width = 32

    def gather(i):
        z_to, first = i // (LANES // width), lax.rem(i, LANES // width) * width
        base = pl.multiple_of(i * width, width)
        for r in range(width):
            source = pl.ds(inverse[z_to, first + r], 1)
            for k, array in enumerate((returns, new, prox)):
                placed[k, pl.ds(base + r, 1), :] = array[source, :]

    pl.loop(0, 12)(gather)

    all_a = bytes_of(got_a.at[pl.ds(0, len(flat))], stat_send.at[0], stat_recv.at[0])
    all_a.wait_recv()
    merged = combine([[got_a[i, k] for k in range(3)] for i in range(2 * plane)])
    for k in range(3):
        msg_b[k] = merged[k]
        got_b[z, k] = merged[k]

    @pl.when(low)
    def _():
        pl.semaphore_wait(here_sem, half)

    for bits in (4, 5, 7, 6, 3, 2, 1):
        pltpu.make_async_remote_copy(
            src_ref=msg_b, dst_ref=got_b.at[z], send_sem=stat_send.at[1], recv_sem=stat_recv.at[1],
            device_id=along(bits), device_id_type=MESH,
        ).start()

    for o in flat:
        if o[0] == 0:
            pltpu.make_async_remote_copy(
                src_ref=packed_count, dst_ref=got_count.at[here], send_sem=count_send.at[0], recv_sem=count_recv.at[0],
                device_id=at(*o), device_id_type=MESH,
            ).start()
    got_count[here] = packed_count[...]

    pl.loop(12, blocks // width)(gather)

    all_b = bytes_of(got_b.at[pl.ds(0, n_z - 1)], stat_send.at[1], stat_recv.at[1])
    all_b.wait_recv()
    count, mean, square = combine([[got_b[i, k] for k in range(3)] for i in range(n_z)])
    scale = 1.0 / jnp.sqrt(square / jnp.maximum(count, 1.0) + 0.05)

    def spread(row, v):
        return jnp.broadcast_to(jnp.sum(jnp.where(lane == v, row, 0.0), axis=1, keepdims=True), (chunk, LANES))

    means = [spread(mean, v) for v in range(VERSIONS)]
    scales = [spread(scale, v) for v in range(VERSIONS)]

    for c in range(n_z):
        rows = pl.ds(c * chunk, chunk)
        tag_c = kinds[rows, :]
        mean_c, scale_c = means[0], scales[0]
        for v in range(1, VERSIONS):
            mean_c = jnp.where(tag_c == v, means[v], mean_c)
            scale_c = jnp.where(tag_c == v, scales[v], scale_c)
        white = (placed[0, rows, :] - mean_c) * scale_c
        factor = jnp.where(white >= 0.0, placed[1, rows, :], placed[2, rows, :])
        loss[rows, :] = -(factor * white)

    own = pl.ds(pl.multiple_of(me * per_peer, per_peer), per_peer)
    steps = [(dz, dy, dx) for dy in FAR4 for dx in FAR4 for dz in FAR8]

    for step in steps[:-1]:
        device = at(0, *step)
        there = (device[1] * plane + device[2] * n_x + device[3]) * per_peer
        pltpu.make_async_remote_copy(
            src_ref=loss.at[pl.ds(pl.multiple_of(there, per_peer), per_peer)], dst_ref=token_o.at[own],
            send_sem=token_send, recv_sem=token_recv.at[z], device_id=device, device_id_type=MESH,
        ).start()
    token_o[own, :] = loss[own, :]

    bytes_of(got_count.at[pl.ds(0, plane - 1)], count_send.at[0], count_recv.at[0]).wait_recv()
    lanes8 = lax.broadcasted_iota(jnp.int32, (n_z, LANES), 1) // per_peer
    gathered = jnp.zeros((n_z, LANES), jnp.float32)
    for p in range(plane):
        turn = lax.rem((p - here + plane) * per_peer, LANES)
        gathered = jnp.where(lanes8 == p, pltpu.roll(got_count[p], turn, 1), gathered)
    for r in range(n_z):
        count_rows[r] = gathered[r : r + 1, :]
    got_rows[z] = count_rows[z]
    for bits in range(1, n_z):
        pltpu.make_async_remote_copy(
            src_ref=count_rows.at[z ^ bits], dst_ref=got_rows.at[z], send_sem=count_send.at[1], recv_sem=count_recv.at[1],
            device_id=along(bits), device_id_type=MESH,
        ).start()

    bytes_of(token_o.at[pl.ds(0, blocks - per_peer)], token_send, token_recv.at[0]).wait_send()
    for dz in (0, 1, 7, 2, 6, 3, 5, 4):
        src = lax.rem(z + dz, n_z)
        expect = blocks // n_z - (per_peer if dz == 0 else 0)
        bytes_of(token_o.at[pl.ds(0, expect)], token_send, token_recv.at[src]).wait_recv()
        rows = pl.ds(pl.multiple_of(src * chunk, chunk), chunk)
        block_o[pl.ds(src, 1), :] = jnp.sum(token_o[rows, :].T, axis=0, keepdims=True)
    bytes_of(got_rows.at[pl.ds(0, n_z - 1)], count_send.at[1], count_recv.at[1]).wait_recv()
    for r in range(n_z):
        block_o[r : r + 1, :] = block_o[r : r + 1, :] / jnp.maximum(got_rows[r], 1.0)

    bytes_of(got_a.at[pl.ds(0, len(flat))], stat_send.at[0], stat_recv.at[0]).wait_send()
    bytes_of(got_b.at[pl.ds(0, n_z - 1)], stat_send.at[1], stat_recv.at[1]).wait_send()
    bytes_of(got_count.at[pl.ds(0, plane - 1)], count_send.at[0], count_recv.at[0]).wait_send()
    bytes_of(got_rows.at[pl.ds(0, n_z - 1)], count_send.at[1], count_recv.at[1]).wait_send()


def store(token_v, block_v, token_o, block_o, sem):
    copies = [pltpu.make_async_copy(token_v, token_o, sem.at[0]), pltpu.make_async_copy(block_v, block_o, sem.at[1])]
    for copy in copies:
        copy.start()
    for copy in copies:
        copy.wait()


def on_device(version_tags, packed_pos, valid_mask, returns, values, log_ratio_new, log_ratio_prox):
    blocks, tokens = valid_mask.shape
    n_z, n_y, n_x = (lax.axis_size(name) for name in AXES[1:])
    plane = n_y * n_x
    f32, i32 = jnp.float32, jnp.int32
    vmem, dma = pltpu.VMEM, pltpu.SemaphoreType.DMA
    small = (blocks // LANES, LANES)
    token_loss, block_loss = pl.pallas_call(
        kernel,
        out_shape=(pltpu.VMEM((blocks, tokens), f32), pltpu.VMEM(small, f32)),
        in_specs=[pl.BlockSpec(memory_space=pltpu.HBM)] * 7,
        out_specs=[pl.BlockSpec(memory_space=pltpu.VMEM)] * 2,
        scratch_shapes=[
            vmem(small, i32), vmem(small, i32), vmem((blocks, tokens), i32),
            *[vmem((blocks, tokens), f32)] * 4,
            vmem((3, *small), f32), vmem(small, i32), vmem((2, blocks, LANES), i32), vmem((blocks, LANES), f32), vmem((3, blocks, LANES), f32), vmem((blocks, LANES), f32),
            vmem(small, i32), pltpu.SMEM(small, i32),
            vmem((3, 1, LANES), f32), vmem((3, 1, LANES), f32), vmem((2 * plane, 3, 1, LANES), f32), vmem((n_z, 3, 1, LANES), f32),
            vmem(small, f32), vmem((plane, *small), f32), vmem((n_z, 1, LANES), f32), vmem((n_z, 1, LANES), f32),
            pltpu.SemaphoreType.REGULAR, dma((12,)), dma((4,)), dma, dma((2,)), dma((2,)), dma((2,)), dma((2,)), dma, dma((n_z,)),
        ],
        compiler_params=pltpu.CompilerParams(collective_id=0, has_side_effects=True, vmem_limit_bytes=32 * 2**20),
    )(*[pltpu.with_memory_space_constraint(a, pltpu.HBM) for a in (version_tags.reshape(small), packed_pos.reshape(small), valid_mask, returns, values, log_ratio_new, log_ratio_prox)])
    token_loss, block_loss = pl.pallas_call(
        store,
        out_shape=(pltpu.HBM((blocks, tokens), f32), pltpu.HBM(small, f32)),
        in_specs=[pl.BlockSpec(memory_space=pltpu.VMEM)] * 2,
        out_specs=[pl.BlockSpec(memory_space=pltpu.HBM)] * 2,
        scratch_shapes=[dma((2,))],
    )(*[pltpu.with_memory_space_constraint(a, pltpu.VMEM) for a in (token_loss, block_loss)])
    return token_loss, block_loss.reshape(blocks)


def solution(mesh):
    split = Mesh(mesh.devices.reshape(mesh.shape["grp"], 8, 4, 4), AXES)
    row, flat = P(AXES, None), P(AXES)
    return jax.shard_map(
        on_device,
        mesh=split,
        in_specs=(flat, flat, row, row, row, row, row),
        out_specs=(row, flat),
        check_vma=False,
    )
```

```python
import functools

import jax
import jax.numpy as jnp
from jax import lax
from jax.experimental import pallas as pl
from jax.experimental.pallas import tpu as pltpu
from jax.sharding import Mesh
from jax.sharding import PartitionSpec as P

MESH = pl.DeviceIdType.MESH
VERSIONS = 4
LANES = 128
AXES = ("grp", "z", "y", "x")
FAR4 = (2, 1, 3, 0)
FAR8 = (4, 3, 5, 2, 6, 1, 7, 0)


def combine(moments):
    count = sum(m[0] for m in moments)
    total = sum(m[0] * m[1] for m in moments)
    mean = total / jnp.maximum(count, 1.0)
    square = sum(m[2] + m[0] * (m[1] - mean) * (m[1] - mean) for m in moments)
    return count, mean, square


def total_of(array):
    return jnp.sum(jnp.sum(array, axis=0, keepdims=True), axis=1, keepdims=True)


def kernel(
    tags_h, packed_h, mask_h, returns_h, values_h, new_h, prox_h,
    token_o, block_o,
    tags, packed, mask, returns, values, new, prox,
    per_block, per_count, keys, kinds, placed, loss, inverse_v, inverse,
    msg_a, msg_b, got_a, got_b,
    packed_count, got_count, count_rows, got_rows,
    here_sem, part_sem, load_sem, scalar_sem, stat_send, stat_recv, count_send, count_recv, token_send, token_recv,
):
    g, z, y, x = (lax.axis_index(name) for name in AXES)
    n_z, n_y, n_x = (lax.axis_size(name) for name in AXES[1:])
    plane = n_y * n_x
    blocks = mask.shape[0]
    chunk = blocks // n_z
    per_peer = blocks // (n_z * plane)
    here = y * n_x + x
    me = z * plane + here

    parts = 2
    part = blocks // parts
    stat_loads = [
        [
            pltpu.make_async_copy(src.at[pl.ds(i * part, part)], dst.at[pl.ds(i * part, part)], part_sem.at[3 * i + k])
            for k, (src, dst) in enumerate([(mask_h, mask), (returns_h, returns), (values_h, values)])
        ]
        for i in range(parts)
    ]
    loads = [
        pltpu.make_async_copy(src, dst, load_sem.at[i])
        for i, (src, dst) in enumerate([(tags_h, tags), (packed_h, packed), (new_h, new), (prox_h, prox)])
    ]
    for load in sum(stat_loads, []) + loads[:2]:
        load.start()

    def at(dg, dz, dy, dx):
        return (g ^ dg, lax.rem(z + dz, n_z), lax.rem(y + dy, n_y), lax.rem(x + dx, n_x))

    flat = [(dg, 0, dy, dx) for dy in FAR4 for dx in FAR4 for dg in (1, 0) if (dg, dy, dx) != (0, 0, 0)]
    half = n_z // 2
    low = z < half

    def along(bits):
        return (g, z ^ bits, y, x)

    barrier = pltpu.get_barrier_semaphore()
    for o in flat:
        pl.semaphore_signal(barrier, inc=1, device_id=at(*o), device_id_type=MESH)
    for bits in range(1, half):
        pl.semaphore_signal(barrier, inc=1, device_id=along(bits), device_id_type=MESH)

    @pl.when(low)
    def _():
        for bits in range(half, n_z):
            pl.semaphore_signal(barrier, inc=1, device_id=along(bits), device_id_type=MESH)

    for s in range(n_z):
        rows = pl.ds(s * chunk, chunk)
        if s * chunk % part == 0:
            for load in stat_loads[s * chunk // part]:
                load.wait()
        valid = mask[rows, :].T
        per_count[s : s + 1, :] = jnp.sum(valid, axis=0, keepdims=True)
        valid = valid.astype(jnp.float32)
        advantage = (returns[rows, :] - values[rows, :]).T
        count = per_count[s : s + 1, :].astype(jnp.float32)
        mean = jnp.sum(valid * advantage, axis=0, keepdims=True) / jnp.maximum(count, 1.0)
        centred = advantage - mean
        per_block[0, s : s + 1, :] = count
        per_block[1, s : s + 1, :] = mean
        per_block[2, s : s + 1, :] = jnp.sum(valid * centred * centred, axis=0, keepdims=True)

    for load in loads[2:]:
        load.start()
    loads[0].wait()
    lane = lax.broadcasted_iota(jnp.int32, (1, LANES), 1)
    tag = tags[...]
    count, mean, square = per_block[0], per_block[1], per_block[2]
    local = [jnp.zeros((1, LANES), jnp.float32)] * 3
    for v in range(VERSIONS):
        mine = tag == v
        count_v = total_of(jnp.where(mine, count, 0.0))
        mean_v = total_of(jnp.where(mine, count * mean, 0.0)) / jnp.maximum(count_v, 1.0)
        square_v = total_of(jnp.where(mine, square + count * (mean - mean_v) * (mean - mean_v), 0.0))
        local = [jnp.where(lane == v, new_value, old) for new_value, old in zip((count_v, mean_v, square_v), local)]
    own_a = g * plane + here
    for k in range(3):
        msg_a[k] = local[k]
        got_a[own_a, k] = local[k]

    pl.semaphore_wait(barrier, len(flat) + half - 1 + jnp.where(low, 0, half))
    for o in flat:
        pltpu.make_async_remote_copy(
            src_ref=msg_a, dst_ref=got_a.at[own_a], send_sem=stat_send.at[0], recv_sem=stat_recv.at[0],
            device_id=at(*o), device_id_type=MESH,
        ).start()

    def bytes_of(ref, send, recv):
        return pltpu.make_async_remote_copy(src_ref=ref, dst_ref=ref, send_sem=send, recv_sem=recv, device_id=(g, z, y, x), device_id_type=MESH)

    @pl.when(jnp.logical_not(low))
    def _():
        for bits in range(half, n_z):
            pl.semaphore_signal(here_sem, inc=1, device_id=along(bits), device_id_type=MESH)

    loads[1].wait()
    where = packed[...]
    order = ((where // blocks) & (n_z * plane - 1)) * per_peer + (where & (blocks - 1)) - me * per_peer
    block = lax.broadcasted_iota(jnp.int32, order.shape, 0) * LANES + lax.broadcasted_iota(jnp.int32, order.shape, 1)
    value = block + blocks * (per_count[...] + 2 * LANES * tag)

    def columns(row):
        return jnp.broadcast_to(row, (chunk, LANES)).T

    for s in range(n_z):
        rows = pl.ds(s * chunk, chunk)
        keys[0, rows, :] = columns(order[s : s + 1, :])
        keys[1, rows, :] = columns(value[s : s + 1, :])
    place = lax.broadcasted_iota(jnp.int32, (chunk, LANES), 1)
    for c in range(n_z):
        total = jnp.zeros((chunk, LANES), jnp.int32)
        for s in range(n_z):
            rows = pl.ds(s * chunk, chunk)
            total = total + jnp.where(keys[0, rows, :] == place + c * LANES, keys[1, rows, :], 0)
        total = jnp.sum(total, axis=0, keepdims=True)
        inverse_v[c : c + 1, :] = total & (blocks - 1)
        packed_count[c : c + 1, :] = ((total // blocks) & (2 * LANES - 1)).astype(jnp.float32)
        kinds[c * chunk : (c + 1) * chunk, :] = columns((total // (2 * LANES * blocks)).astype(jnp.float32))
    to_scalar = pltpu.make_async_copy(inverse_v, inverse, scalar_sem)
    to_scalar.start()

    for o in flat:
        if o[0] == 0:
            pltpu.make_async_remote_copy(
                src_ref=packed_count, dst_ref=got_count.at[here], send_sem=count_send.at[0], recv_sem=count_recv.at[0],
                device_id=at(*o), device_id_type=MESH,
            ).start()
    got_count[here] = packed_count[...]

    for load in loads[2:]:
        load.wait()
    for s in range(n_z):
        rows = pl.ds(s * chunk, chunk)
        ratio = jnp.exp(new[rows, :])
        weight = mask[rows, :].astype(jnp.float32) * jnp.exp(prox[rows, :])
        new[rows, :] = weight * jnp.minimum(ratio, 1.2)
        prox[rows, :] = weight * jnp.maximum(ratio, 0.8)
        returns[rows, :] = returns[rows, :] - values[rows, :]

    to_scalar.wait()
    width = 32

    def gather(i):
        z_to, first = i // (LANES // width), lax.rem(i, LANES // width) * width
        base = pl.multiple_of(i * width, width)
        for r in range(width):
            source = pl.ds(inverse[z_to, first + r], 1)
            for k, array in enumerate((returns, new, prox)):
                placed[k, pl.ds(base + r, 1), :] = array[source, :]

    pl.loop(0, 12)(gather)

    all_a = bytes_of(got_a.at[pl.ds(0, len(flat))], stat_send.at[0], stat_recv.at[0])
    all_a.wait_recv()
    merged = combine([[got_a[i, k] for k in range(3)] for i in range(2 * plane)])
    for k in range(3):
        msg_b[k] = merged[k]
        got_b[z, k] = merged[k]

    @pl.when(low)
    def _():
        pl.semaphore_wait(here_sem, half)

    for bits in (4, 5, 7, 6, 3, 2, 1):
        pltpu.make_async_remote_copy(
            src_ref=msg_b, dst_ref=got_b.at[z], send_sem=stat_send.at[1], recv_sem=stat_recv.at[1],
            device_id=along(bits), device_id_type=MESH,
        ).start()

    pl.loop(12, blocks // width)(gather)

    bytes_of(got_count.at[pl.ds(0, plane - 1)], count_send.at[0], count_recv.at[0]).wait_recv()
    lanes8 = lax.broadcasted_iota(jnp.int32, (n_z, LANES), 1) // per_peer
    gathered = jnp.zeros((n_z, LANES), jnp.float32)
    for p in range(plane):
        turn = lax.rem((p - here + plane) * per_peer, LANES)
        gathered = jnp.where(lanes8 == p, pltpu.roll(got_count[p], turn, 1), gathered)
    for r in range(n_z):
        count_rows[r] = gathered[r : r + 1, :]
    got_rows[z] = count_rows[z]
    for bits in range(1, n_z):
        pltpu.make_async_remote_copy(
            src_ref=count_rows.at[z ^ bits], dst_ref=got_rows.at[z], send_sem=count_send.at[1], recv_sem=count_recv.at[1],
            device_id=along(bits), device_id_type=MESH,
        ).start()

    all_b = bytes_of(got_b.at[pl.ds(0, n_z - 1)], stat_send.at[1], stat_recv.at[1])
    all_b.wait_recv()
    count, mean, square = combine([[got_b[i, k] for k in range(3)] for i in range(n_z)])
    scale = 1.0 / jnp.sqrt(square / jnp.maximum(count, 1.0) + 0.05)

    def spread(row, v):
        return jnp.broadcast_to(jnp.sum(jnp.where(lane == v, row, 0.0), axis=1, keepdims=True), (strip, LANES))

    strip = chunk // n_y
    means = [spread(mean, v) for v in range(VERSIONS)]
    scales = [spread(scale, v) for v in range(VERSIONS)]

    own = pl.ds(pl.multiple_of(me * per_peer, per_peer), per_peer)

    def finish(dy):
        for c in range(n_z):
            rows = pl.ds(pl.multiple_of(c * chunk + ((y + dy) & (n_y - 1)) * strip, strip), strip)
            tag_c = kinds[rows, :]
            mean_c, scale_c = means[0], scales[0]
            for v in range(1, VERSIONS):
                mean_c = jnp.where(tag_c == v, means[v], mean_c)
                scale_c = jnp.where(tag_c == v, scales[v], scale_c)
            white = (placed[0, rows, :] - mean_c) * scale_c
            factor = jnp.where(white >= 0.0, placed[1, rows, :], placed[2, rows, :])
            loss[rows, :] = -(factor * white)

    def send(dy):
        for dx in FAR4:
            for dz in FAR8:
                if (dz, dy, dx) != (0, 0, 0):
                    device = at(0, dz, dy, dx)
                    there = (device[1] * plane + device[2] * n_x + device[3]) * per_peer
                    pltpu.make_async_remote_copy(
                        src_ref=loss.at[pl.ds(pl.multiple_of(there, per_peer), per_peer)], dst_ref=token_o.at[own],
                        send_sem=token_send, recv_sem=token_recv.at[z], device_id=device, device_id_type=MESH,
                    ).start()

    finish(FAR4[0])
    finish(FAR4[1])
    send(FAR4[0])
    finish(FAR4[2])
    send(FAR4[1])
    finish(FAR4[3])
    send(FAR4[2])
    send(FAR4[3])
    token_o[own, :] = loss[own, :]

    bytes_of(token_o.at[pl.ds(0, blocks - per_peer)], token_send, token_recv.at[0]).wait_send()
    for dz in (0, 1, 7, 2, 6, 3, 5, 4):
        src = lax.rem(z + dz, n_z)
        expect = blocks // n_z - (per_peer if dz == 0 else 0)
        bytes_of(token_o.at[pl.ds(0, expect)], token_send, token_recv.at[src]).wait_recv()
        rows = pl.ds(pl.multiple_of(src * chunk, chunk), chunk)
        block_o[pl.ds(src, 1), :] = jnp.sum(token_o[rows, :].T, axis=0, keepdims=True)
    bytes_of(got_rows.at[pl.ds(0, n_z - 1)], count_send.at[1], count_recv.at[1]).wait_recv()
    for r in range(n_z):
        block_o[r : r + 1, :] = block_o[r : r + 1, :] / jnp.maximum(got_rows[r], 1.0)

    bytes_of(got_a.at[pl.ds(0, len(flat))], stat_send.at[0], stat_recv.at[0]).wait_send()
    bytes_of(got_b.at[pl.ds(0, n_z - 1)], stat_send.at[1], stat_recv.at[1]).wait_send()
    bytes_of(got_count.at[pl.ds(0, plane - 1)], count_send.at[0], count_recv.at[0]).wait_send()
    bytes_of(got_rows.at[pl.ds(0, n_z - 1)], count_send.at[1], count_recv.at[1]).wait_send()


def store(token_v, block_v, token_o, block_o, sem):
    copies = [pltpu.make_async_copy(token_v, token_o, sem.at[0]), pltpu.make_async_copy(block_v, block_o, sem.at[1])]
    for copy in copies:
        copy.start()
    for copy in copies:
        copy.wait()


def on_device(version_tags, packed_pos, valid_mask, returns, values, log_ratio_new, log_ratio_prox):
    blocks, tokens = valid_mask.shape
    n_z, n_y, n_x = (lax.axis_size(name) for name in AXES[1:])
    plane = n_y * n_x
    f32, i32 = jnp.float32, jnp.int32
    vmem, dma = pltpu.VMEM, pltpu.SemaphoreType.DMA
    small = (blocks // LANES, LANES)
    token_loss, block_loss = pl.pallas_call(
        kernel,
        out_shape=(pltpu.VMEM((blocks, tokens), f32), pltpu.VMEM(small, f32)),
        in_specs=[pl.BlockSpec(memory_space=pltpu.HBM)] * 7,
        out_specs=[pl.BlockSpec(memory_space=pltpu.VMEM)] * 2,
        scratch_shapes=[
            vmem(small, i32), vmem(small, i32), vmem((blocks, tokens), i32),
            *[vmem((blocks, tokens), f32)] * 4,
            vmem((3, *small), f32), vmem(small, i32), vmem((2, blocks, LANES), i32), vmem((blocks, LANES), f32), vmem((3, blocks, LANES), f32), vmem((blocks, LANES), f32),
            vmem(small, i32), pltpu.SMEM(small, i32),
            vmem((3, 1, LANES), f32), vmem((3, 1, LANES), f32), vmem((2 * plane, 3, 1, LANES), f32), vmem((n_z, 3, 1, LANES), f32),
            vmem(small, f32), vmem((plane, *small), f32), vmem((n_z, 1, LANES), f32), vmem((n_z, 1, LANES), f32),
            pltpu.SemaphoreType.REGULAR, dma((6,)), dma((4,)), dma, dma((2,)), dma((2,)), dma((2,)), dma((2,)), dma, dma((n_z,)),
        ],
        compiler_params=pltpu.CompilerParams(collective_id=0, has_side_effects=True, vmem_limit_bytes=32 * 2**20),
    )(*[pltpu.with_memory_space_constraint(a, pltpu.HBM) for a in (version_tags.reshape(small), packed_pos.reshape(small), valid_mask, returns, values, log_ratio_new, log_ratio_prox)])
    token_loss, block_loss = pl.pallas_call(
        store,
        out_shape=(pltpu.HBM((blocks, tokens), f32), pltpu.HBM(small, f32)),
        in_specs=[pl.BlockSpec(memory_space=pltpu.VMEM)] * 2,
        out_specs=[pl.BlockSpec(memory_space=pltpu.HBM)] * 2,
        scratch_shapes=[dma((2,))],
    )(*[pltpu.with_memory_space_constraint(a, pltpu.VMEM) for a in (token_loss, block_loss)])
    return token_loss, block_loss.reshape(blocks)


def solution(mesh):
    split = Mesh(mesh.devices.reshape(mesh.shape["grp"], 8, 4, 4), AXES)
    row, flat = P(AXES, None), P(AXES)
    return jax.shard_map(
        on_device,
        mesh=split,
        in_specs=(flat, flat, row, row, row, row, row),
        out_specs=(row, flat),
        check_vma=False,
    )
```

```python
import functools

import jax
import jax.numpy as jnp
from jax import lax
from jax.experimental import pallas as pl
from jax.experimental.pallas import tpu as pltpu
from jax.sharding import Mesh
from jax.sharding import PartitionSpec as P

MESH = pl.DeviceIdType.MESH
VERSIONS = 4
LANES = 128
AXES = ("grp", "z", "y", "x")
FAR4 = (2, 1, 3, 0)
FAR8 = (4, 3, 5, 2, 6, 1, 7, 0)


def combine(moments):
    count = sum(m[0] for m in moments)
    total = sum(m[0] * m[1] for m in moments)
    mean = total / jnp.maximum(count, 1.0)
    square = sum(m[2] + m[0] * (m[1] - mean) * (m[1] - mean) for m in moments)
    return count, mean, square


def total_of(array):
    return jnp.sum(jnp.sum(array, axis=0, keepdims=True), axis=1, keepdims=True)


def kernel(
    tags_h, packed_h, mask_h, returns_h, values_h, new_h, prox_h,
    token_o, block_o,
    tags, packed, mask, returns, values, new, prox,
    per_block, per_count, keys, kinds, placed, loss, inverse_v, inverse,
    msg_a, msg_b, got_a, got_b,
    packed_count, got_count, count_rows, got_rows,
    here_sem, part_sem, load_sem, scalar_sem, stat_send, stat_recv, count_send, count_recv, token_send, token_recv,
):
    g, z, y, x = (lax.axis_index(name) for name in AXES)
    n_z, n_y, n_x = (lax.axis_size(name) for name in AXES[1:])
    plane = n_y * n_x
    blocks = mask.shape[0]
    chunk = blocks // n_z
    per_peer = blocks // (n_z * plane)
    here = y * n_x + x
    me = z * plane + here

    parts = 2
    part = blocks // parts
    stat_loads = [
        [
            pltpu.make_async_copy(src.at[pl.ds(i * part, part)], dst.at[pl.ds(i * part, part)], part_sem.at[3 * i + k])
            for k, (src, dst) in enumerate([(mask_h, mask), (returns_h, returns), (values_h, values)])
        ]
        for i in range(parts)
    ]
    loads = [
        pltpu.make_async_copy(src, dst, load_sem.at[i])
        for i, (src, dst) in enumerate([(tags_h, tags), (packed_h, packed), (new_h, new), (prox_h, prox)])
    ]
    for load in sum(stat_loads, []) + loads[:2]:
        load.start()

    def at(dg, dz, dy, dx):
        return (g ^ dg, lax.rem(z + dz, n_z), lax.rem(y + dy, n_y), lax.rem(x + dx, n_x))

    flat = [(dg, 0, dy, dx) for dy in FAR4 for dx in FAR4 for dg in (1, 0) if (dg, dy, dx) != (0, 0, 0)]
    half = n_z // 2
    low = z < half

    def along(bits):
        return (g, z ^ bits, y, x)

    barrier = pltpu.get_barrier_semaphore()
    for o in flat:
        pl.semaphore_signal(barrier, inc=1, device_id=at(*o), device_id_type=MESH)
    for bits in range(1, half):
        pl.semaphore_signal(barrier, inc=1, device_id=along(bits), device_id_type=MESH)

    @pl.when(low)
    def _():
        for bits in range(half, n_z):
            pl.semaphore_signal(barrier, inc=1, device_id=along(bits), device_id_type=MESH)

    for s in range(n_z):
        rows = pl.ds(s * chunk, chunk)
        if s * chunk % part == 0:
            for load in stat_loads[s * chunk // part]:
                load.wait()
        valid = mask[rows, :].T
        per_count[s : s + 1, :] = jnp.sum(valid, axis=0, keepdims=True)
        valid = valid.astype(jnp.float32)
        advantage = (returns[rows, :] - values[rows, :]).T
        count = per_count[s : s + 1, :].astype(jnp.float32)
        mean = jnp.sum(valid * advantage, axis=0, keepdims=True) / jnp.maximum(count, 1.0)
        centred = advantage - mean
        per_block[0, s : s + 1, :] = count
        per_block[1, s : s + 1, :] = mean
        per_block[2, s : s + 1, :] = jnp.sum(valid * centred * centred, axis=0, keepdims=True)

    for load in loads[2:]:
        load.start()
    loads[0].wait()
    lane = lax.broadcasted_iota(jnp.int32, (1, LANES), 1)
    tag = tags[...]
    count, mean, square = per_block[0], per_block[1], per_block[2]
    local = [jnp.zeros((1, LANES), jnp.float32)] * 3
    for v in range(VERSIONS):
        mine = tag == v
        count_v = total_of(jnp.where(mine, count, 0.0))
        mean_v = total_of(jnp.where(mine, count * mean, 0.0)) / jnp.maximum(count_v, 1.0)
        square_v = total_of(jnp.where(mine, square + count * (mean - mean_v) * (mean - mean_v), 0.0))
        local = [jnp.where(lane == v, new_value, old) for new_value, old in zip((count_v, mean_v, square_v), local)]
    own_a = g * plane + here
    for k in range(3):
        msg_a[k] = local[k]
        got_a[own_a, k] = local[k]

    pl.semaphore_wait(barrier, len(flat) + half - 1 + jnp.where(low, 0, half))
    for o in flat:
        pltpu.make_async_remote_copy(
            src_ref=msg_a, dst_ref=got_a.at[own_a], send_sem=stat_send.at[0], recv_sem=stat_recv.at[0],
            device_id=at(*o), device_id_type=MESH,
        ).start()

    def bytes_of(ref, send, recv):
        return pltpu.make_async_remote_copy(src_ref=ref, dst_ref=ref, send_sem=send, recv_sem=recv, device_id=(g, z, y, x), device_id_type=MESH)

    @pl.when(jnp.logical_not(low))
    def _():
        for bits in range(half, n_z):
            pl.semaphore_signal(here_sem, inc=1, device_id=along(bits), device_id_type=MESH)

    loads[1].wait()
    where = packed[...]
    order = ((where // blocks) & (n_z * plane - 1)) * per_peer + (where & (blocks - 1)) - me * per_peer
    block = lax.broadcasted_iota(jnp.int32, order.shape, 0) * LANES + lax.broadcasted_iota(jnp.int32, order.shape, 1)
    value = block + blocks * (per_count[...] + 2 * LANES * tag)

    def columns(row):
        return jnp.broadcast_to(row, (chunk, LANES)).T

    for s in range(n_z):
        rows = pl.ds(s * chunk, chunk)
        keys[0, rows, :] = columns(order[s : s + 1, :])
        keys[1, rows, :] = columns(value[s : s + 1, :])
    place = lax.broadcasted_iota(jnp.int32, (chunk, LANES), 1)
    for c in range(n_z):
        total = jnp.zeros((chunk, LANES), jnp.int32)
        for s in range(n_z):
            rows = pl.ds(s * chunk, chunk)
            total = total + jnp.where(keys[0, rows, :] == place + c * LANES, keys[1, rows, :], 0)
        total = jnp.sum(total, axis=0, keepdims=True)
        inverse_v[c : c + 1, :] = total & (blocks - 1)
        packed_count[c : c + 1, :] = ((total // blocks) & (2 * LANES - 1)).astype(jnp.float32)
        kinds[c * chunk : (c + 1) * chunk, :] = columns((total // (2 * LANES * blocks)).astype(jnp.float32))
    to_scalar = pltpu.make_async_copy(inverse_v, inverse, scalar_sem)
    to_scalar.start()

    for o in flat:
        if o[0] == 0:
            pltpu.make_async_remote_copy(
                src_ref=packed_count, dst_ref=got_count.at[here], send_sem=count_send.at[0], recv_sem=count_recv.at[0],
                device_id=at(*o), device_id_type=MESH,
            ).start()
    got_count[here] = packed_count[...]

    for load in loads[2:]:
        load.wait()
    for s in range(n_z):
        rows = pl.ds(s * chunk, chunk)
        ratio = jnp.exp(new[rows, :])
        weight = mask[rows, :].astype(jnp.float32) * jnp.exp(prox[rows, :])
        new[rows, :] = weight * jnp.minimum(ratio, 1.2)
        prox[rows, :] = weight * jnp.maximum(ratio, 0.8)
        returns[rows, :] = returns[rows, :] - values[rows, :]

    to_scalar.wait()
    width = 32

    def gather(i):
        z_to, first = i // (LANES // width), lax.rem(i, LANES // width) * width
        base = pl.multiple_of(i * width, width)
        for r in range(width):
            source = pl.ds(inverse[z_to, first + r], 1)
            for k, array in enumerate((returns, new, prox)):
                placed[k, pl.ds(base + r, 1), :] = array[source, :]

    pl.loop(0, 12)(gather)

    all_a = bytes_of(got_a.at[pl.ds(0, len(flat))], stat_send.at[0], stat_recv.at[0])
    all_a.wait_recv()
    merged = combine([[got_a[i, k] for k in range(3)] for i in range(2 * plane)])
    for k in range(3):
        msg_b[k] = merged[k]
        got_b[z, k] = merged[k]

    @pl.when(low)
    def _():
        pl.semaphore_wait(here_sem, half)

    for bits in (4, 5, 7, 6, 3, 2, 1):
        pltpu.make_async_remote_copy(
            src_ref=msg_b, dst_ref=got_b.at[z], send_sem=stat_send.at[1], recv_sem=stat_recv.at[1],
            device_id=along(bits), device_id_type=MESH,
        ).start()

    pl.loop(12, blocks // width)(gather)

    bytes_of(got_count.at[pl.ds(0, plane - 1)], count_send.at[0], count_recv.at[0]).wait_recv()
    lanes8 = lax.broadcasted_iota(jnp.int32, (n_z, LANES), 1) // per_peer
    gathered = jnp.zeros((n_z, LANES), jnp.float32)
    for p in range(plane):
        turn = lax.rem((p - here + plane) * per_peer, LANES)
        gathered = jnp.where(lanes8 == p, pltpu.roll(got_count[p], turn, 1), gathered)
    for r in range(n_z):
        count_rows[r] = gathered[r : r + 1, :]
    got_rows[z] = count_rows[z]
    for bits in range(1, n_z):
        pltpu.make_async_remote_copy(
            src_ref=count_rows.at[z ^ bits], dst_ref=got_rows.at[z], send_sem=count_send.at[1], recv_sem=count_recv.at[1],
            device_id=along(bits), device_id_type=MESH,
        ).start()

    all_b = bytes_of(got_b.at[pl.ds(0, n_z - 1)], stat_send.at[1], stat_recv.at[1])
    all_b.wait_recv()
    count, mean, square = combine([[got_b[i, k] for k in range(3)] for i in range(n_z)])
    scale = 1.0 / jnp.sqrt(square / jnp.maximum(count, 1.0) + 0.05)

    def spread(row, v):
        return jnp.broadcast_to(jnp.sum(jnp.where(lane == v, row, 0.0), axis=1, keepdims=True), (strip, LANES))

    strip = chunk // n_y
    means = [spread(mean, v) for v in range(VERSIONS)]
    scales = [spread(scale, v) for v in range(VERSIONS)]

    own = pl.ds(pl.multiple_of(me * per_peer, per_peer), per_peer)

    def finish(dy):
        for c in range(n_z):
            rows = pl.ds(pl.multiple_of(c * chunk + ((y + dy) & (n_y - 1)) * strip, strip), strip)
            tag_c = kinds[rows, :]
            mean_c, scale_c = means[0], scales[0]
            for v in range(1, VERSIONS):
                mean_c = jnp.where(tag_c == v, means[v], mean_c)
                scale_c = jnp.where(tag_c == v, scales[v], scale_c)
            white = (placed[0, rows, :] - mean_c) * scale_c
            factor = jnp.where(white >= 0.0, placed[1, rows, :], placed[2, rows, :])
            loss[rows, :] = -(factor * white)

    def send(dy):
        for dx in FAR4:
            for dz in FAR8:
                if (dz, dy, dx) != (0, 0, 0):
                    device = at(0, dz, dy, dx)
                    there = (device[1] * plane + device[2] * n_x + device[3]) * per_peer
                    pltpu.make_async_remote_copy(
                        src_ref=loss.at[pl.ds(pl.multiple_of(there, per_peer), per_peer)], dst_ref=token_o.at[own],
                        send_sem=token_send, recv_sem=token_recv.at[z], device_id=device, device_id_type=MESH,
                    ).start()

    finish(FAR4[0])
    finish(FAR4[1])
    send(FAR4[0])
    finish(FAR4[2])
    send(FAR4[1])
    finish(FAR4[3])
    send(FAR4[2])
    send(FAR4[3])
    token_o[own, :] = loss[own, :]

    bytes_of(got_rows.at[pl.ds(0, n_z - 1)], count_send.at[1], count_recv.at[1]).wait_recv()
    for together in ((0,), (1, 7), (2, 6), (3, 5, 4)):
        sources = [lax.rem(z + dz, n_z) for dz in together]
        for dz, src in zip(together, sources):
            expect = blocks // n_z - (per_peer if dz == 0 else 0)
            bytes_of(token_o.at[pl.ds(0, expect)], token_send, token_recv.at[src]).wait_recv()
        arrived = [token_o[pl.ds(pl.multiple_of(src * chunk, chunk), chunk), :] for src in sources]
        sums = [jnp.sum(rows.T, axis=0, keepdims=True) for rows in arrived]
        for src, total in zip(sources, sums):
            block_o[pl.ds(src, 1), :] = total / jnp.maximum(got_rows[src], 1.0)
    bytes_of(token_o.at[pl.ds(0, blocks - per_peer)], token_send, token_recv.at[0]).wait_send()
    bytes_of(got_a.at[pl.ds(0, len(flat))], stat_send.at[0], stat_recv.at[0]).wait_send()
    bytes_of(got_b.at[pl.ds(0, n_z - 1)], stat_send.at[1], stat_recv.at[1]).wait_send()
    bytes_of(got_count.at[pl.ds(0, plane - 1)], count_send.at[0], count_recv.at[0]).wait_send()
    bytes_of(got_rows.at[pl.ds(0, n_z - 1)], count_send.at[1], count_recv.at[1]).wait_send()


def store(token_v, block_v, token_o, block_o, sem):
    copies = [pltpu.make_async_copy(token_v, token_o, sem.at[0]), pltpu.make_async_copy(block_v, block_o, sem.at[1])]
    for copy in copies:
        copy.start()
    for copy in copies:
        copy.wait()


def on_device(version_tags, packed_pos, valid_mask, returns, values, log_ratio_new, log_ratio_prox):
    blocks, tokens = valid_mask.shape
    n_z, n_y, n_x = (lax.axis_size(name) for name in AXES[1:])
    plane = n_y * n_x
    f32, i32 = jnp.float32, jnp.int32
    vmem, dma = pltpu.VMEM, pltpu.SemaphoreType.DMA
    small = (blocks // LANES, LANES)
    token_loss, block_loss = pl.pallas_call(
        kernel,
        out_shape=(pltpu.VMEM((blocks, tokens), f32), pltpu.VMEM(small, f32)),
        in_specs=[pl.BlockSpec(memory_space=pltpu.HBM)] * 7,
        out_specs=[pl.BlockSpec(memory_space=pltpu.VMEM)] * 2,
        scratch_shapes=[
            vmem(small, i32), vmem(small, i32), vmem((blocks, tokens), i32),
            *[vmem((blocks, tokens), f32)] * 4,
            vmem((3, *small), f32), vmem(small, i32), vmem((2, blocks, LANES), i32), vmem((blocks, LANES), f32), vmem((3, blocks, LANES), f32), vmem((blocks, LANES), f32),
            vmem(small, i32), pltpu.SMEM(small, i32),
            vmem((3, 1, LANES), f32), vmem((3, 1, LANES), f32), vmem((2 * plane, 3, 1, LANES), f32), vmem((n_z, 3, 1, LANES), f32),
            vmem(small, f32), vmem((plane, *small), f32), vmem((n_z, 1, LANES), f32), vmem((n_z, 1, LANES), f32),
            pltpu.SemaphoreType.REGULAR, dma((6,)), dma((4,)), dma, dma((2,)), dma((2,)), dma((2,)), dma((2,)), dma, dma((n_z,)),
        ],
        compiler_params=pltpu.CompilerParams(collective_id=0, has_side_effects=True, vmem_limit_bytes=32 * 2**20),
    )(*[pltpu.with_memory_space_constraint(a, pltpu.HBM) for a in (version_tags.reshape(small), packed_pos.reshape(small), valid_mask, returns, values, log_ratio_new, log_ratio_prox)])
    token_loss, block_loss = pl.pallas_call(
        store,
        out_shape=(pltpu.HBM((blocks, tokens), f32), pltpu.HBM(small, f32)),
        in_specs=[pl.BlockSpec(memory_space=pltpu.VMEM)] * 2,
        out_specs=[pl.BlockSpec(memory_space=pltpu.HBM)] * 2,
        scratch_shapes=[dma((2,))],
    )(*[pltpu.with_memory_space_constraint(a, pltpu.VMEM) for a in (token_loss, block_loss)])
    return token_loss, block_loss.reshape(blocks)


def solution(mesh):
    split = Mesh(mesh.devices.reshape(mesh.shape["grp"], 8, 4, 4), AXES)
    row, flat = P(AXES, None), P(AXES)
    return jax.shard_map(
        on_device,
        mesh=split,
        in_specs=(flat, flat, row, row, row, row, row),
        out_specs=(row, flat),
        check_vma=False,
    )
```

```python
import functools

import jax
import jax.numpy as jnp
from jax import lax
from jax.experimental import pallas as pl
from jax.experimental.pallas import tpu as pltpu
from jax.sharding import Mesh
from jax.sharding import PartitionSpec as P

MESH = pl.DeviceIdType.MESH
VERSIONS = 4
LANES = 128
AXES = ("grp", "z", "y", "x")
FAR4 = (2, 1, 3, 0)
FAR8 = (4, 3, 5, 2, 6, 1, 7, 0)


def combine(moments):
    count = sum(m[0] for m in moments)
    total = sum(m[0] * m[1] for m in moments)
    mean = total / jnp.maximum(count, 1.0)
    square = sum(m[2] + m[0] * (m[1] - mean) * (m[1] - mean) for m in moments)
    return count, mean, square


def total_of(array):
    return jnp.sum(jnp.sum(array, axis=0, keepdims=True), axis=1, keepdims=True)


def kernel(
    tags_h, packed_h, mask_h, returns_h, values_h, new_h, prox_h,
    token_o, block_o,
    tags, packed, mask, returns, values, new, prox,
    per_block, per_count, keys, kinds, placed, loss, inverse_v, inverse,
    msg_a, msg_b, got_a, got_b,
    packed_count, got_count, count_rows, got_rows,
    here_sem, part_sem, load_sem, scalar_sem, stat_send, stat_recv, count_send, count_recv, token_send, token_recv,
):
    g, z, y, x = (lax.axis_index(name) for name in AXES)
    n_z, n_y, n_x = (lax.axis_size(name) for name in AXES[1:])
    plane = n_y * n_x
    blocks = mask.shape[0]
    chunk = blocks // n_z
    per_peer = blocks // (n_z * plane)
    here = y * n_x + x
    me = z * plane + here

    parts = 2
    part = blocks // parts
    stat_loads = [
        [
            pltpu.make_async_copy(src.at[pl.ds(i * part, part)], dst.at[pl.ds(i * part, part)], part_sem.at[3 * i + k])
            for k, (src, dst) in enumerate([(mask_h, mask), (returns_h, returns), (values_h, values)])
        ]
        for i in range(parts)
    ]
    loads = [
        pltpu.make_async_copy(src, dst, load_sem.at[i])
        for i, (src, dst) in enumerate([(tags_h, tags), (packed_h, packed), (new_h, new), (prox_h, prox)])
    ]
    for load in sum(stat_loads, []) + loads[:2]:
        load.start()

    def at(dg, dz, dy, dx):
        return (g ^ dg, lax.rem(z + dz, n_z), lax.rem(y + dy, n_y), lax.rem(x + dx, n_x))

    flat = [(dg, 0, dy, dx) for dy in FAR4 for dx in FAR4 for dg in (1, 0) if (dg, dy, dx) != (0, 0, 0)]
    half = n_z // 2
    low = z < half

    def along(bits):
        return (g, z ^ bits, y, x)

    barrier = pltpu.get_barrier_semaphore()
    for o in flat:
        pl.semaphore_signal(barrier, inc=1, device_id=at(*o), device_id_type=MESH)
    for bits in range(1, half):
        pl.semaphore_signal(barrier, inc=1, device_id=along(bits), device_id_type=MESH)

    @pl.when(low)
    def _():
        for bits in range(half, n_z):
            pl.semaphore_signal(barrier, inc=1, device_id=along(bits), device_id_type=MESH)

    for s in range(n_z):
        rows = pl.ds(s * chunk, chunk)
        if s * chunk % part == 0:
            for load in stat_loads[s * chunk // part]:
                load.wait()
        valid = mask[rows, :].T
        per_count[s : s + 1, :] = jnp.sum(valid, axis=0, keepdims=True)
        valid = valid.astype(jnp.float32)
        advantage = (returns[rows, :] - values[rows, :]).T
        count = per_count[s : s + 1, :].astype(jnp.float32)
        mean = jnp.sum(valid * advantage, axis=0, keepdims=True) / jnp.maximum(count, 1.0)
        centred = advantage - mean
        per_block[0, s : s + 1, :] = count
        per_block[1, s : s + 1, :] = mean
        per_block[2, s : s + 1, :] = jnp.sum(valid * centred * centred, axis=0, keepdims=True)

    for load in loads[2:]:
        load.start()
    loads[0].wait()
    lane = lax.broadcasted_iota(jnp.int32, (1, LANES), 1)
    tag = tags[...]
    count, mean, square = per_block[0], per_block[1], per_block[2]
    local = [jnp.zeros((1, LANES), jnp.float32)] * 3
    stacked = [jnp.sum(jnp.where(tag == v, part, 0.0), axis=0, keepdims=True) for part in (count, count * mean) for v in range(VERSIONS)]
    totals = jnp.sum(jnp.concatenate(stacked, axis=0), axis=1, keepdims=True)
    for v in range(VERSIONS):
        mine = tag == v
        count_v = totals[v : v + 1, :]
        mean_v = totals[VERSIONS + v : VERSIONS + v + 1, :] / jnp.maximum(count_v, 1.0)
        square_v = total_of(jnp.where(mine, square + count * (mean - mean_v) * (mean - mean_v), 0.0))
        local = [jnp.where(lane == v, new_value, old) for new_value, old in zip((count_v, mean_v, square_v), local)]
    own_a = g * plane + here
    for k in range(3):
        msg_a[k] = local[k]
        got_a[own_a, k] = local[k]

    pl.semaphore_wait(barrier, len(flat) + half - 1 + jnp.where(low, 0, half))
    for o in flat:
        pltpu.make_async_remote_copy(
            src_ref=msg_a, dst_ref=got_a.at[own_a], send_sem=stat_send.at[0], recv_sem=stat_recv.at[0],
            device_id=at(*o), device_id_type=MESH,
        ).start()

    def bytes_of(ref, send, recv):
        return pltpu.make_async_remote_copy(src_ref=ref, dst_ref=ref, send_sem=send, recv_sem=recv, device_id=(g, z, y, x), device_id_type=MESH)

    @pl.when(jnp.logical_not(low))
    def _():
        for bits in range(half, n_z):
            pl.semaphore_signal(here_sem, inc=1, device_id=along(bits), device_id_type=MESH)

    loads[1].wait()
    where = packed[...]
    order = ((where // blocks) & (n_z * plane - 1)) * per_peer + (where & (blocks - 1)) - me * per_peer
    block = lax.broadcasted_iota(jnp.int32, order.shape, 0) * LANES + lax.broadcasted_iota(jnp.int32, order.shape, 1)
    value = block + blocks * (per_count[...] + 2 * LANES * tag)

    def columns(row):
        return jnp.broadcast_to(row, (chunk, LANES)).T

    for s in range(n_z):
        rows = pl.ds(s * chunk, chunk)
        keys[0, rows, :] = columns(order[s : s + 1, :])
        keys[1, rows, :] = columns(value[s : s + 1, :])
    place = lax.broadcasted_iota(jnp.int32, (chunk, LANES), 1)
    for c in range(n_z):
        total = jnp.zeros((chunk, LANES), jnp.int32)
        for s in range(n_z):
            rows = pl.ds(s * chunk, chunk)
            total = total + jnp.where(keys[0, rows, :] == place + c * LANES, keys[1, rows, :], 0)
        total = jnp.sum(total, axis=0, keepdims=True)
        inverse_v[c : c + 1, :] = total & (blocks - 1)
        packed_count[c : c + 1, :] = ((total // blocks) & (2 * LANES - 1)).astype(jnp.float32)
        kinds[c * chunk : (c + 1) * chunk, :] = columns((total // (2 * LANES * blocks)).astype(jnp.float32))
    to_scalar = pltpu.make_async_copy(inverse_v, inverse, scalar_sem)
    to_scalar.start()

    for o in flat:
        if o[0] == 0:
            pltpu.make_async_remote_copy(
                src_ref=packed_count, dst_ref=got_count.at[here], send_sem=count_send.at[0], recv_sem=count_recv.at[0],
                device_id=at(*o), device_id_type=MESH,
            ).start()
    got_count[here] = packed_count[...]

    for load in loads[2:]:
        load.wait()
    for s in range(n_z):
        rows = pl.ds(s * chunk, chunk)
        ratio = jnp.exp(new[rows, :])
        weight = mask[rows, :].astype(jnp.float32) * jnp.exp(prox[rows, :])
        new[rows, :] = weight * jnp.minimum(ratio, 1.2)
        prox[rows, :] = weight * jnp.maximum(ratio, 0.8)
        returns[rows, :] = returns[rows, :] - values[rows, :]

    to_scalar.wait()
    width = 32

    def gather(i):
        z_to, first = i // (LANES // width), lax.rem(i, LANES // width) * width
        base = pl.multiple_of(i * width, width)
        for r in range(width):
            source = pl.ds(inverse[z_to, first + r], 1)
            for k, array in enumerate((returns, new, prox)):
                placed[k, pl.ds(base + r, 1), :] = array[source, :]

    pl.loop(0, 12)(gather)

    all_a = bytes_of(got_a.at[pl.ds(0, len(flat))], stat_send.at[0], stat_recv.at[0])
    all_a.wait_recv()
    merged = combine([[got_a[i, k] for k in range(3)] for i in range(2 * plane)])
    for k in range(3):
        msg_b[k] = merged[k]
        got_b[z, k] = merged[k]

    @pl.when(low)
    def _():
        pl.semaphore_wait(here_sem, half)

    for bits in (4, 5, 7, 6, 3, 2, 1):
        pltpu.make_async_remote_copy(
            src_ref=msg_b, dst_ref=got_b.at[z], send_sem=stat_send.at[1], recv_sem=stat_recv.at[1],
            device_id=along(bits), device_id_type=MESH,
        ).start()

    pl.loop(12, blocks // width)(gather)

    bytes_of(got_count.at[pl.ds(0, plane - 1)], count_send.at[0], count_recv.at[0]).wait_recv()
    lanes8 = lax.broadcasted_iota(jnp.int32, (n_z, LANES), 1) // per_peer
    gathered = jnp.zeros((n_z, LANES), jnp.float32)
    for p in range(plane):
        turn = lax.rem((p - here + plane) * per_peer, LANES)
        gathered = jnp.where(lanes8 == p, pltpu.roll(got_count[p], turn, 1), gathered)
    for r in range(n_z):
        count_rows[r] = gathered[r : r + 1, :]
    got_rows[z] = count_rows[z]
    for bits in range(1, n_z):
        pltpu.make_async_remote_copy(
            src_ref=count_rows.at[z ^ bits], dst_ref=got_rows.at[z], send_sem=count_send.at[1], recv_sem=count_recv.at[1],
            device_id=along(bits), device_id_type=MESH,
        ).start()

    all_b = bytes_of(got_b.at[pl.ds(0, n_z - 1)], stat_send.at[1], stat_recv.at[1])
    all_b.wait_recv()
    count, mean, square = combine([[got_b[i, k] for k in range(3)] for i in range(n_z)])
    scale = 1.0 / jnp.sqrt(square / jnp.maximum(count, 1.0) + 0.05)

    def spread(row, v):
        return jnp.broadcast_to(jnp.sum(jnp.where(lane == v, row, 0.0), axis=1, keepdims=True), (strip, LANES))

    strip = chunk // n_y
    means = [spread(mean, v) for v in range(VERSIONS)]
    scales = [spread(scale, v) for v in range(VERSIONS)]

    own = pl.ds(pl.multiple_of(me * per_peer, per_peer), per_peer)

    def finish(dy):
        for c in range(n_z):
            rows = pl.ds(pl.multiple_of(c * chunk + ((y + dy) & (n_y - 1)) * strip, strip), strip)
            tag_c = kinds[rows, :]
            mean_c, scale_c = means[0], scales[0]
            for v in range(1, VERSIONS):
                mean_c = jnp.where(tag_c == v, means[v], mean_c)
                scale_c = jnp.where(tag_c == v, scales[v], scale_c)
            white = (placed[0, rows, :] - mean_c) * scale_c
            factor = jnp.where(white >= 0.0, placed[1, rows, :], placed[2, rows, :])
            loss[rows, :] = -(factor * white)

    def send(dy):
        for dx in FAR4:
            for dz in FAR8:
                if (dz, dy, dx) != (0, 0, 0):
                    device = at(0, dz, dy, dx)
                    there = (device[1] * plane + device[2] * n_x + device[3]) * per_peer
                    pltpu.make_async_remote_copy(
                        src_ref=loss.at[pl.ds(pl.multiple_of(there, per_peer), per_peer)], dst_ref=token_o.at[own],
                        send_sem=token_send, recv_sem=token_recv.at[z], device_id=device, device_id_type=MESH,
                    ).start()

    finish(FAR4[0])
    finish(FAR4[1])
    send(FAR4[0])
    finish(FAR4[2])
    send(FAR4[1])
    finish(FAR4[3])
    send(FAR4[2])
    send(FAR4[3])
    token_o[own, :] = loss[own, :]

    bytes_of(got_rows.at[pl.ds(0, n_z - 1)], count_send.at[1], count_recv.at[1]).wait_recv()
    for together in ((0,), (1, 7), (2, 6), (3, 5, 4)):
        sources = [lax.rem(z + dz, n_z) for dz in together]
        for dz, src in zip(together, sources):
            expect = blocks // n_z - (per_peer if dz == 0 else 0)
            bytes_of(token_o.at[pl.ds(0, expect)], token_send, token_recv.at[src]).wait_recv()
        arrived = [token_o[pl.ds(pl.multiple_of(src * chunk, chunk), chunk), :] for src in sources]
        sums = [jnp.sum(rows.T, axis=0, keepdims=True) for rows in arrived]
        for src, total in zip(sources, sums):
            block_o[pl.ds(src, 1), :] = total / jnp.maximum(got_rows[src], 1.0)
    bytes_of(token_o.at[pl.ds(0, blocks - per_peer)], token_send, token_recv.at[0]).wait_send()
    bytes_of(got_a.at[pl.ds(0, len(flat))], stat_send.at[0], stat_recv.at[0]).wait_send()
    bytes_of(got_b.at[pl.ds(0, n_z - 1)], stat_send.at[1], stat_recv.at[1]).wait_send()
    bytes_of(got_count.at[pl.ds(0, plane - 1)], count_send.at[0], count_recv.at[0]).wait_send()
    bytes_of(got_rows.at[pl.ds(0, n_z - 1)], count_send.at[1], count_recv.at[1]).wait_send()


def store(token_v, block_v, token_o, block_o, sem):
    copies = [pltpu.make_async_copy(token_v, token_o, sem.at[0]), pltpu.make_async_copy(block_v, block_o, sem.at[1])]
    for copy in copies:
        copy.start()
    for copy in copies:
        copy.wait()


def on_device(version_tags, packed_pos, valid_mask, returns, values, log_ratio_new, log_ratio_prox):
    blocks, tokens = valid_mask.shape
    n_z, n_y, n_x = (lax.axis_size(name) for name in AXES[1:])
    plane = n_y * n_x
    f32, i32 = jnp.float32, jnp.int32
    vmem, dma = pltpu.VMEM, pltpu.SemaphoreType.DMA
    small = (blocks // LANES, LANES)
    token_loss, block_loss = pl.pallas_call(
        kernel,
        out_shape=(pltpu.VMEM((blocks, tokens), f32), pltpu.VMEM(small, f32)),
        in_specs=[pl.BlockSpec(memory_space=pltpu.HBM)] * 7,
        out_specs=[pl.BlockSpec(memory_space=pltpu.VMEM)] * 2,
        scratch_shapes=[
            vmem(small, i32), vmem(small, i32), vmem((blocks, tokens), i32),
            *[vmem((blocks, tokens), f32)] * 4,
            vmem((3, *small), f32), vmem(small, i32), vmem((2, blocks, LANES), i32), vmem((blocks, LANES), f32), vmem((3, blocks, LANES), f32), vmem((blocks, LANES), f32),
            vmem(small, i32), pltpu.SMEM(small, i32),
            vmem((3, 1, LANES), f32), vmem((3, 1, LANES), f32), vmem((2 * plane, 3, 1, LANES), f32), vmem((n_z, 3, 1, LANES), f32),
            vmem(small, f32), vmem((plane, *small), f32), vmem((n_z, 1, LANES), f32), vmem((n_z, 1, LANES), f32),
            pltpu.SemaphoreType.REGULAR, dma((6,)), dma((4,)), dma, dma((2,)), dma((2,)), dma((2,)), dma((2,)), dma, dma((n_z,)),
        ],
        compiler_params=pltpu.CompilerParams(collective_id=0, has_side_effects=True, vmem_limit_bytes=32 * 2**20),
    )(*[pltpu.with_memory_space_constraint(a, pltpu.HBM) for a in (version_tags.reshape(small), packed_pos.reshape(small), valid_mask, returns, values, log_ratio_new, log_ratio_prox)])
    token_loss, block_loss = pl.pallas_call(
        store,
        out_shape=(pltpu.HBM((blocks, tokens), f32), pltpu.HBM(small, f32)),
        in_specs=[pl.BlockSpec(memory_space=pltpu.VMEM)] * 2,
        out_specs=[pl.BlockSpec(memory_space=pltpu.HBM)] * 2,
        scratch_shapes=[dma((2,))],
    )(*[pltpu.with_memory_space_constraint(a, pltpu.VMEM) for a in (token_loss, block_loss)])
    return token_loss, block_loss.reshape(blocks)


def solution(mesh):
    split = Mesh(mesh.devices.reshape(mesh.shape["grp"], 8, 4, 4), AXES)
    row, flat = P(AXES, None), P(AXES)
    return jax.shard_map(
        on_device,
        mesh=split,
        in_specs=(flat, flat, row, row, row, row, row),
        out_specs=(row, flat),
        check_vma=False,
    )
```
